32 devices in a mesh: member: 4 (over x, core), region: 8 (over z, y).
Axes of the slice: x: 2, y: 2, z: 4, core: 2. Of those that a mesh axis runs over, the one named last changes fastest.
Arguments:
- ensemble: float32 [12, 16, 32, 512], P('member', 'region'), may hold values from -6 to 6
- obs_value: float32 [16, 32, 128], P(None, ('member', 'region')), may hold values from -6 to 6
- obs_error: float32 [16, 32, 128], P(None, ('member', 'region')), may hold values from 0.5 to 4
- obs_index: int32 [16, 32, 128], P(None, ('member', 'region')), may hold values from 0 to 511
- obs_count: int32 [16, 32], P(None, ('member', 'region')), may hold values from 1 to 128
Outputs:
- analysis: float32 [12, 16, 32, 512], P('member', 'region')
The draws below stay inside these ranges and needn't reach their ends.
Inputs may be any that keep to these rules, and one draw needn't show every extreme that they name: `obs_index`: value v names field v // (256) (0 SST, 1 SSH) at cell v mod (256) of the block, cells row-major. `obs_count`: slots below a block's count are observations; the others are padding and carry no weight.
All inputs are finite; a program needn't handle non-finite values.
Results may differ from the reference program's by a relative error of at most 0.0001.
Values sent between devices are 32-bit elements; how exact they have to be, the bound alone decides.
A program may use at most 64 MiB of HBM per device.

```python
import math
import jax
import jax.numpy as jnp
from jax import lax

SIDE = 16
OBS = 128
NS_ITERS = 6
VALS = 512
MEMBERS = 12
BROWS = 16
BCOLS = 32


def set_ends(values, own_key, low, high):
    shape = values.shape
    place = [jax.random.randint(jax.random.fold_in(own_key, axis), (), 0, shape[axis]) for axis in range(len(shape))]
    values = values.at[tuple(place)].set(low)
    longest = shape.index(max(shape))
    place[longest] = (place[longest] + 1) % shape[longest]
    return values.at[tuple(place)].set(high)


def steps_of(key, extent, cuts, smallest, top_value):
    def one(dim, shards_of):
        draws = jax.random.uniform(jax.random.fold_in(jax.random.fold_in(key, 6), dim), (shards_of,), jnp.float32, smallest / len(cuts), top_value / len(cuts))
        return jnp.repeat(jnp.exp(draws), extent[dim] // shards_of).reshape((-1,) + (1,) * (len(extent) - dim - 1))

    loudness = one(*cuts[0])
    for cut in cuts[1:]:
        loudness = loudness * one(*cut)
    return loudness


def normal_values(key, shape, width, bound, shards=(), kind=jnp.bfloat16):
    result = jax.random.normal(key, shape, jnp.float32) * width
    if len(shards) > 0:
        result = steps_of(key, shape, shards, -0.22, 0.18) * result
    return jnp.clip(result, min=-bound, max=bound).astype(kind)


def setup_inputs(seed: int = 0) -> dict:
    streams_of = jax.random.split(jax.random.key(seed), 6)
    ensemble = normal_values(streams_of[0], (MEMBERS, BROWS, BCOLS, VALS), 1.0, 6.0, ((0, 4), (1, 8)), jnp.float32)
    obs_value = normal_values(streams_of[1], (BROWS, BCOLS, OBS), 1.0, 6.0, ((1, 32),), jnp.float32)
    obs_error = jnp.clip(jnp.exp(math.log(4.0) - 2.0794415 * jax.random.uniform(streams_of[2], (BROWS, BCOLS, OBS), jnp.float32) ** steps_of(streams_of[2], (BROWS, BCOLS, OBS), ((1, 32),), -0.2, 0.2)), 0.5, 4.0)
    obs_index = set_ends(jax.random.randint(streams_of[3], (BROWS, BCOLS, OBS), 0, VALS), jax.random.fold_in(streams_of[3], 1), 0, VALS - 1).astype(jnp.int32)
    obs_count = set_ends(jax.random.randint(streams_of[4], (BROWS, BCOLS), 1, OBS + 1), jax.random.fold_in(streams_of[4], 1), 1, OBS).astype(jnp.int32)
    return dict(ensemble=ensemble, obs_value=obs_value, obs_error=obs_error, obs_index=obs_index, obs_count=obs_count)


LOC_SCALE = 12.0
INFLATION_FACTOR = 1.1

def batch_product(left, right):
    return jnp.einsum('...ij,...jk->...ik', left, right, precision=lax.Precision.HIGHEST)

def observe(ensemble, obs_value, obs_error, obs_index, obs_count):
    ens_mean = lax.optimization_barrier(jnp.mean(ensemble, axis=0))
    anomaly = ensemble - ens_mean
    slot_index = lax.broadcasted_iota(jnp.int32, obs_index.shape, 2)
    live_slot = jnp.where(slot_index < obs_count[:, :, None], 1.0, 0.0).astype(jnp.float32)
    root_weight = jnp.sqrt(live_slot / obs_error)
    full_index = jnp.broadcast_to(obs_index[None], (anomaly.shape[0],) + obs_index.shape).astype(jnp.int32)
    seen_anom = jnp.take_along_axis(anomaly, full_index, axis=3)
    seen_mean = jnp.take_along_axis(ens_mean, obs_index.astype(jnp.int32), axis=2)
    rescaled_values = root_weight[:, :, None] * jnp.moveaxis(seen_anom, 0, 2)
    innovation = root_weight * (obs_value - seen_mean)
    cell_index = obs_index % (SIDE * SIDE)
    rowpos = (cell_index // SIDE).astype(jnp.float32)
    column_position = (cell_index % SIDE).astype(jnp.float32)
    stacked = jnp.concatenate([rescaled_values, innovation[:, :, None], rowpos[:, :, None], column_position[:, :, None]], axis=2)
    return (anomaly, ens_mean, stacked)

def analyze(anomaly, ens_mean, padded):
    ensemble_members = anomaly.shape[0]
    row_count = anomaly.shape[1]
    col_count = anomaly.shape[2]
    pieces = []
    for row_step in range(3):
        for col_step in range(3):
            pieces.append(padded[row_step:row_step + row_count, col_step:col_step + col_count])
    nearby = jnp.stack(pieces, axis=2)
    rescaled_values = nearby[:, :, :, :ensemble_members]
    innovation = nearby[:, :, :, ensemble_members]
    rowpos = nearby[:, :, :, ensemble_members + 1]
    column_position = nearby[:, :, :, ensemble_members + 2]
    offset_index = jnp.arange(9, dtype=jnp.int32)
    offset_row = (offset_index // 3 - 1).astype(jnp.float32) * SIDE
    offset_col = (offset_index % 3 - 1).astype(jnp.float32) * SIDE
    half_side = SIDE // 2
    point_index = jnp.arange(4, dtype=jnp.int32)
    center_row = (point_index // 2).astype(jnp.float32) * half_side + (half_side - 1) * 0.5
    center_col = (point_index % 2).astype(jnp.float32) * half_side + (half_side - 1) * 0.5
    row_gap = offset_row[:, None] + rowpos
    col_gap = offset_col[:, None] + column_position
    distance = (row_gap[:, :, None] - center_row[:, None, None]) ** 2 + (col_gap[:, :, None] - center_col[:, None, None]) ** 2
    locality = jnp.exp(-distance / (2.0 * LOC_SCALE * LOC_SCALE))
    weighted = locality[:, :, :, :, None, :] * rescaled_values[:, :, None]
    gramian_total = jnp.einsum('rcpnko,rcnjo->rcpkj', weighted, rescaled_values, precision=lax.Precision.HIGHEST)
    drive_vec = jnp.einsum('rcpnko,rcno->rcpk', weighted, innovation, precision=lax.Precision.HIGHEST)
    identity_matrix = jnp.eye(ensemble_members, dtype=jnp.float32)
    precision_matrix = gramian_total + (ensemble_members - 1) / INFLATION_FACTOR * identity_matrix
    norm_scale = jnp.sqrt(lax.optimization_barrier(jnp.sum(precision_matrix * precision_matrix, axis=(3, 4), keepdims=True)))
    root_iter = precision_matrix / norm_scale
    inv_iter = jnp.broadcast_to(identity_matrix, precision_matrix.shape)
    for sweep_index in range(NS_ITERS):
        ns_step = 1.5 * identity_matrix - 0.5 * batch_product(inv_iter, root_iter)
        root_iter = batch_product(root_iter, ns_step)
        inv_iter = batch_product(ns_step, inv_iter)
    inv_root = inv_iter / jnp.sqrt(norm_scale)
    half_way = jnp.einsum('rcpkj,rcpj->rcpk', inv_root, drive_vec, precision=lax.Precision.HIGHEST)
    mean_w = jnp.einsum('rcpkj,rcpj->rcpk', inv_root, half_way, precision=lax.Precision.HIGHEST)
    weights = mean_w[..., :, None] + math.sqrt(ensemble_members - 1) * inv_root
    point_weights = weights.reshape(row_count, col_count, 2, 2, ensemble_members, ensemble_members)
    shaped = anomaly.reshape(ensemble_members, row_count, col_count, 2, 2, half_side, 2, half_side)
    updated = jnp.einsum('jrcvaybx,rcabjk->krcvaybx', shaped, point_weights, precision=lax.Precision.HIGHEST)
    return ens_mean[None] + updated.reshape(anomaly.shape)

def reference(ensemble, obs_value, obs_error, obs_index, obs_count):
    anomaly, ens_mean, stacked = observe(ensemble, obs_value, obs_error, obs_index, obs_count)
    padded = jnp.pad(stacked, ((1, 1), (1, 1), (0, 0), (0, 0)))

    def one_row(row_index):
        part_anom = lax.dynamic_slice_in_dim(anomaly, row_index, 1, 1)
        part_mean = lax.dynamic_slice_in_dim(ens_mean, row_index, 1, 0)
        part_pad = lax.dynamic_slice_in_dim(padded, row_index, 3, 0)
        return analyze(part_anom, part_mean, part_pad)
    row_results = lax.map(one_row, jnp.arange(BROWS, dtype=jnp.int32))
    return jnp.moveaxis(row_results[:, :, 0], 0, 1)
```

```python
import functools
import math

import jax
import jax.numpy as jnp
from jax import lax
from jax.experimental import pallas as pl
from jax.experimental.pallas import tpu as pltpu
from jax.sharding import PartitionSpec as P

SIDE = 16
CELLS = SIDE * SIDE
HALF = SIDE // 2
LANES = 128
NS_ITERS = 6
LOC_SCALE = 12.0
INFLATION_FACTOR = 1.1
MESH = pl.DeviceIdType.MESH
NT = (((1,), (1,)), ((), ()))


def up_to(value, step):
    return -(-value // step) * step


def split(values):
    high = values.astype(jnp.bfloat16)
    low = (values - high.astype(jnp.float32)).astype(jnp.bfloat16)
    return high, low


def kernel(
    dims,
    ens_ref, value_ref, error_ref, index_ref, count_ref, out_ref,
    ens, pack, obs, mean, slots, place, loc, qhi, qlo, acc, side,
    row_in, side_in, prec, root, inv, step, small, weights, outgoing,
    ens_send, ens_recv, obs_send, obs_recv, halo_send, halo_recv, out_send, out_recv, local_sem,
):
    M, G, K, R, C, V, O, J, QP = dims
    members = M * K
    m = lax.axis_index("member")
    g = lax.axis_index("region")
    pack_rows = pack.shape[0] // G
    ts = 2 * (R + 2)
    targets = 4 * C * (R + 2)
    f32 = jnp.float32

    barrier = pltpu.get_barrier_semaphore()
    for off in range(1, M):
        pl.semaphore_signal(barrier, inc=1, device_id=(lax.rem(m + off, M), g), device_id_type=MESH)
    for off in range(1, G):
        pl.semaphore_signal(barrier, inc=1, device_id=(m, lax.rem(g + off, G)), device_id_type=MESH)
    near = {}
    for dm in (-1, 0, 1):
        for dg in (-1, 0, 1):
            if dm == 0 and dg == 0:
                continue
            ok = jnp.bool_(True)
            if dm:
                ok = jnp.logical_and(ok, m > 0 if dm < 0 else m < M - 1)
            if dg:
                ok = jnp.logical_and(ok, g > 0 if dg < 0 else g < G - 1)
            near[dm, dg] = ok
            if dm and dg:
                @pl.when(ok)
                def _():
                    pl.semaphore_signal(barrier, inc=1, device_id=(m + dm, g + dg), device_id_type=MESH)

    own_ens = pltpu.make_async_copy(
        ens_ref.at[:, :, pl.ds(pl.multiple_of(m * C, C), C), :], ens.at[pl.ds(m * K, K)], local_sem.at[0]
    )
    own_ens.start()
    slot = lax.broadcasted_iota(jnp.int32, (G * R, O), 1)
    slot_row = lax.broadcasted_iota(jnp.int32, (G * R, O), 0)
    count = jnp.zeros((G * R, O), jnp.int32)
    for d in range(G * R):
        count = jnp.where(slot_row == d, count_ref[0, d], count)
    live = jnp.where(slot < count, 1.0, 0.0).astype(f32)
    weight = jnp.sqrt(live / error_ref[...])
    value = value_ref[...]
    index_f = index_ref[...].astype(f32)
    for d in range(G):
        base = d * pack_rows
        pack[base : base + R, :] = weight[d * R : (d + 1) * R]
        pack[base + R : base + 2 * R, :] = value[d * R : (d + 1) * R]
        pack[base + 2 * R : base + 3 * R, :] = index_f[d * R : (d + 1) * R]
        if pack_rows > 3 * R:
            pack[base + 3 * R : base + pack_rows, :] = jnp.zeros((pack_rows - 3 * R, O), f32)
    if QP > members * J:
        qhi[members * J :, :] = jnp.zeros((QP - members * J, qhi.shape[1]), jnp.bfloat16)
        qlo[members * J :, :] = jnp.zeros((QP - members * J, qlo.shape[1]), jnp.bfloat16)

    sides = jnp.where(m > 0, 1, 0) + jnp.where(m < M - 1, 1, 0)
    ends = jnp.where(g > 0, 1, 0) + jnp.where(g < G - 1, 1, 0)
    pl.semaphore_wait(barrier, M - 1 + G - 1 + sides * ends)

    sends = []
    for off in range(1, M):
        to = lax.rem(m + off, M)
        copy = pltpu.make_async_remote_copy(
            src_ref=ens_ref.at[:, :, pl.ds(pl.multiple_of(to * C, C), C), :],
            dst_ref=ens.at[pl.ds(m * K, K)],
            send_sem=ens_send.at[off], recv_sem=ens_recv.at[off],
            device_id=(to, g), device_id_type=MESH,
        )
        copy.start()
        sends.append(copy)
    own_row = pl.ds(pl.multiple_of(g * pack_rows, pack_rows), pack_rows)
    own_obs = pltpu.make_async_copy(pack.at[own_row], obs.at[own_row], local_sem.at[1])
    own_obs.start()
    for off in range(1, G):
        to = lax.rem(g + off, G)
        copy = pltpu.make_async_remote_copy(
            src_ref=pack.at[pl.ds(pl.multiple_of(to * pack_rows, pack_rows), pack_rows)],
            dst_ref=obs.at[own_row],
            send_sem=obs_send.at[off], recv_sem=obs_recv.at[off],
            device_id=(m, to), device_id_type=MESH,
        )
        copy.start()
        sends.append(copy)
    own_ens.wait()
    own_obs.wait()
    for off in range(1, M):
        came = lax.rem(m + M - off, M)
        pltpu.make_async_remote_copy(
            src_ref=ens_ref.at[:, :, pl.ds(pl.multiple_of(m * C, C), C), :],
            dst_ref=ens.at[pl.ds(came * K, K)],
            send_sem=ens_send.at[off], recv_sem=ens_recv.at[off],
            device_id=(came, g), device_id_type=MESH,
        ).wait_recv()
    for off in range(1, G):
        came = lax.rem(g + G - off, G)
        pltpu.make_async_remote_copy(
            src_ref=pack.at[own_row],
            dst_ref=obs.at[pl.ds(pl.multiple_of(came * pack_rows, pack_rows), pack_rows)],
            send_sem=obs_send.at[off], recv_sem=obs_recv.at[off],
            device_id=(m, came), device_id_type=MESH,
        ).wait_recv()

    tiles = V // LANES
    for i in range(R):
        wgt = obs[pl.ds(i, C, stride=pack_rows), :]
        val = obs[pl.ds(R + i, C, stride=pack_rows), :]
        idx = obs[pl.ds(2 * R + i, C, stride=pack_rows), :].astype(jnp.int32)
        lane = idx & (LANES - 1)
        tile = idx >> 7
        cell = idx & (CELLS - 1)
        place[2 * i] = (cell >> 4).astype(f32)
        place[2 * i + 1] = (cell & (SIDE - 1)).astype(f32)

        def seen(rows):
            got = jnp.take_along_axis(rows[:, :LANES], lane, axis=1)
            for t in range(1, tiles):
                more = jnp.take_along_axis(rows[:, t * LANES : (t + 1) * LANES], lane, axis=1)
                got = jnp.where(tile == t, more, got)
            return got

        total = ens[0, i]
        for k in range(1, members):
            total = total + ens[k, i]
        avg = total * (1.0 / members)
        mean[i] = avg
        seen_mean = seen(avg)
        base = i * J * C
        for k in range(members):
            slots[base + k * C : base + (k + 1) * C, :] = wgt * (seen(ens[k, i]) - seen_mean)
        slots[base + members * C : base + (members + 1) * C, :] = wgt * (val - seen_mean)
        if J > members + 1:
            slots[base + (members + 1) * C : base + J * C, :] = jnp.zeros(((J - members - 1) * C, O), f32)

    scale = -1.0 / (2.0 * LOC_SCALE * LOC_SCALE)
    middle = (HALF - 1) * 0.5
    t_id = lax.broadcasted_iota(jnp.int32, (ts, O), 0)
    t_row = t_id >> 1
    t_mid = (t_id & 1).astype(f32) * HALF + middle
    col = lax.broadcasted_iota(jnp.int32, (C, O), 0)
    edges = {0: [None] * R, 1: [None] * R}
    for c in range(C):
        for i in range(R):
            at = (c * R + i) * O
            here = slots[pl.ds(i * J * C + c, J, stride=C), :]
            prod = jnp.concatenate([here[k : k + 1] * here for k in range(members)], axis=0)
            high, low = split(prod)
            qhi[0 : members * J, at : at + O] = high
            qlo[0 : members * J, at : at + O] = low
            y = place[2 * i, c : c + 1, :]
            x = place[2 * i + 1, c : c + 1, :]
            row_off = i + 1 - t_row
            dy = (row_off * SIDE).astype(f32) + y - t_mid
            ly = jnp.where(jnp.abs(row_off) <= 1, jnp.exp(dy * dy * scale), 0.0)
            col_off = c - col
            lx = []
            for pc in range(2):
                dx = (col_off * SIDE).astype(f32) + x - (pc * HALF + middle)
                lx.append(jnp.where(jnp.abs(col_off) <= 1, jnp.exp(dx * dx * scale), 0.0))
            grid = jnp.concatenate([ly[s : s + 1] * lx[pc] for s in range(ts) for pc in range(2)], axis=0)
            high, low = split(grid)
            loc[0:targets, at : at + O] = high
            loc[targets : 2 * targets, at : at + O] = low
            for which, away, at_col in ((0, 1, 0), (1, -1, C - 1)):
                if c == at_col:
                    parts = []
                    for pc in range(2):
                        dx = away * SIDE + x - (pc * HALF + middle)
                        parts.append(ly * jnp.exp(dx * dx * scale))
                    edges[which][i] = jnp.concatenate(parts, axis=0)

    def dot(left, right):
        return lax.dot_general(left, right, NT, preferred_element_type=f32)

    for which, first in ((0, 0), (1, (C - 1) * R * O)):
        high, low = split(jnp.concatenate(edges[which], axis=1))
        hq = qhi[:, first : first + R * O]
        side[which] = dot(high, hq) + dot(low, hq) + dot(high, qlo[:, first : first + R * O])
    both = dot(loc[...], qhi[...])
    acc[...] = both[:targets] + both[targets:] + dot(loc[0:targets, :], qlo[...])

    rows = 4 * C
    plans = []
    for n, (dm, dg) in enumerate(near):
        if dm == 0:
            first = 0 if dg < 0 else (R + 1) * rows
            src = acc.at[first : first + rows]
            dst = row_in.at[0 if dg < 0 else 1]
        else:
            src = side.at[0 if dm < 0 else 1]
            dst = side_in.at[(0 if dm < 0 else 3) + dg + 1]
        plans.append((dm, dg, src, dst, n))
    for dm, dg, src, dst, n in plans:
        @pl.when(near[dm, dg])
        def _():
            pltpu.make_async_remote_copy(
                src_ref=src, dst_ref=dst, send_sem=halo_send.at[n], recv_sem=halo_recv.at[n],
                device_id=(m + dm, g + dg), device_id_type=MESH,
            ).start()
    for dm, dg, src, dst, n in plans:
        @pl.when(near[-dm, -dg])
        def _():
            pltpu.make_async_remote_copy(
                src_ref=src, dst_ref=dst, send_sem=halo_send.at[n], recv_sem=halo_recv.at[n],
                device_id=(m - dm, g - dg), device_id_type=MESH,
            ).wait_recv()

        @pl.when(jnp.logical_not(near[-dm, -dg]))
        def _():
            dst[...] = jnp.zeros(dst.shape, f32)

    sub = lax.broadcasted_iota(jnp.int32, (C, QP), 0)
    own = R * rows
    for i in range(R):
        for pr in range(2):
            for pc in range(2):
                first = (i * 4 + pr * 2 + pc) * C
                block = acc[rows + first : rows + first + C, :]
                if i == R - 1:
                    block = block + row_in[0, (pr * 2 + pc) * C : (pr * 2 + pc + 1) * C, :]
                if i == 0:
                    block = block + row_in[1, (pr * 2 + pc) * C : (pr * 2 + pc + 1) * C, :]
                for base, at_col in ((0, C - 1), (3, 0)):
                    def pick(dg, t):
                        place_in = pc * ts + t * 2 + pr
                        return side_in[base + dg + 1, place_in : place_in + 1, :]

                    line = pick(0, i + 1)
                    if i == R - 1:
                        line = line + pick(-1, 0)
                    if i == 0:
                        line = line + pick(1, R + 1)
                    block = block + jnp.where(sub == at_col, line, 0.0)
                prec[first : first + C, :] = block
    width = prec.shape[0]
    if width > own:
        prec[own:, :] = jnp.zeros((width - own, QP), f32)

    flat = jnp.transpose(prec[...])
    j_id = lax.broadcasted_iota(jnp.int32, (J, width), 0)
    eye = [jnp.where(j_id == k, 1.0, 0.0).astype(f32) for k in range(members)]
    drive = []
    mats = []
    squares = None
    for k in range(members):
        line = flat[k * J : (k + 1) * J]
        drive.append(line[members : members + 1])
        mat = jnp.where(j_id < members, line, 0.0) + ((members - 1) / INFLATION_FACTOR) * eye[k]
        mats.append(mat)
        squares = mat * mat if squares is None else squares + mat * mat
    norm = jnp.sqrt(jnp.sum(squares, axis=0, keepdims=True))
    for k in range(members):
        start = mats[k] / norm
        first_m = 1.5 * eye[k] - 0.5 * start
        root[k] = start
        step[k] = first_m
        inv[k] = first_m

    def times(left, k, right):
        out = left[k, 0:1, :] * right[0]
        for i in range(1, members):
            out = out + left[k, i : i + 1, :] * right[i]
        return out

    def apply(*lefts):
        right = [step[i] for i in range(members)]
        for k in range(members):
            for left in lefts:
                left[k] = times(left, k, right)

    def next_step():
        right = [root[i] for i in range(members)]
        for k in range(members):
            step[k] = 1.5 * jnp.where(j_id == k, 1.0, 0.0) - 0.5 * times(inv, k, right)

    apply(root)

    def sweep(_, carry):
        next_step()
        apply(root, inv)
        return carry

    lax.fori_loop(0, NS_ITERS - 2, sweep, 0)
    next_step()
    apply(inv)
    shrink = 1.0 / jnp.sqrt(norm)
    inv_root = [inv[k] * shrink for k in range(members)]
    half_way = drive[0] * inv_root[0]
    for i in range(1, members):
        half_way = half_way + drive[i] * inv_root[i]
    small[0] = half_way
    mean_w = small[0, 0:1, :] * inv_root[0]
    for i in range(1, members):
        mean_w = mean_w + small[0, i : i + 1, :] * inv_root[i]
    small[1] = mean_w
    for j in range(members):
        weights[j * J : (j + 1) * J, :] = small[1, j : j + 1, :] + math.sqrt(members - 1) * inv_root[j]
    if QP > members * J:
        weights[members * J :, :] = jnp.zeros((QP - members * J, width), f32)
    prec[...] = jnp.transpose(weights[...])

    fields = V // CELLS
    band = HALF * SIDE
    left_half = (lax.broadcasted_iota(jnp.int32, (C, band), 1) & (SIDE - 1)) < HALF
    for dest in range(M):
        for i in range(R):
            for h in range(2):
                first = (i * 4 + 2 * h) * C
                west = prec[first : first + C, :]
                east = prec[first + C : first + 2 * C, :]
                lanes = [f * CELLS + h * band for f in range(fields)]
                avgs = [mean[i, :, a : a + band] for a in lanes]
                outs = [[avgs[f] for f in range(fields)] for _ in range(K)]
                for j in range(members):
                    anoms = [ens[j, i, :, a : a + band] - avgs[f] for f, a in enumerate(lanes)]
                    for kk in range(K):
                        q = j * J + dest * K + kk
                        w = jnp.where(
                            left_half,
                            jnp.broadcast_to(west[:, q : q + 1], (C, band)),
                            jnp.broadcast_to(east[:, q : q + 1], (C, band)),
                        )
                        for f in range(fields):
                            outs[kk][f] = outs[kk][f] + anoms[f] * w
                for kk in range(K):
                    for f, a in enumerate(lanes):
                        outgoing[dest * K + kk, i, :, a : a + band] = outs[kk][f]
        away = lax.rem(dest - m + M, M)
        target = out_ref.at[:, :, pl.ds(pl.multiple_of(m * C, C), C), :]

        @pl.when(away != 0)
        def _():
            pltpu.make_async_remote_copy(
                src_ref=outgoing.at[dest * K : (dest + 1) * K], dst_ref=target,
                send_sem=out_send.at[away], recv_sem=out_recv.at[away],
                device_id=(dest, g), device_id_type=MESH,
            ).start()

        @pl.when(away == 0)
        def _():
            pltpu.make_async_copy(outgoing.at[dest * K : (dest + 1) * K], target, local_sem.at[2]).start()

    for copy in sends:
        copy.wait_send()
    for dm, dg, src, dst, n in plans:
        @pl.when(near[dm, dg])
        def _():
            pltpu.make_async_remote_copy(
                src_ref=src, dst_ref=dst, send_sem=halo_send.at[n], recv_sem=halo_recv.at[n],
                device_id=(m + dm, g + dg), device_id_type=MESH,
            ).wait_send()
    pltpu.make_async_copy(
        outgoing.at[pl.ds(m * K, K)], out_ref.at[:, :, pl.ds(pl.multiple_of(m * C, C), C), :], local_sem.at[2]
    ).wait()
    for off in range(1, M):
        to = lax.rem(m + off, M)
        came = lax.rem(m + M - off, M)
        pltpu.make_async_remote_copy(
            src_ref=outgoing.at[pl.ds(to * K, K)],
            dst_ref=out_ref.at[:, :, pl.ds(pl.multiple_of(came * C, C), C), :],
            send_sem=out_send.at[off], recv_sem=out_recv.at[off],
            device_id=(to, g), device_id_type=MESH,
        ).wait()


def local(M, G, ensemble, obs_value, obs_error, obs_index, obs_count):
    K, R, cols, V = ensemble.shape
    O = obs_value.shape[2]
    C = cols // M
    members = M * K
    J = up_to(members + 1, 8)
    QP = up_to(members * J, LANES)
    slots_all = R * C * O
    targets = 4 * C * (R + 2)
    width = up_to(4 * C * R, LANES)
    pack_rows = up_to(3 * R, 8)
    f32 = jnp.float32
    vmem = pltpu.VMEM
    edge_rows = 4 * (R + 2)
    dma = pltpu.SemaphoreType.DMA
    flat = lambda a: a.reshape(a.shape[0], -1)
    return pl.pallas_call(
        functools.partial(kernel, (M, G, K, R, C, V, O, J, QP)),
        out_shape=jax.ShapeDtypeStruct(ensemble.shape, f32),
        in_specs=[pl.BlockSpec(memory_space=pl.ANY)] + [pl.BlockSpec(memory_space=vmem)] * 3
        + [pl.BlockSpec(memory_space=pltpu.SMEM)],
        out_specs=pl.BlockSpec(memory_space=vmem),
        scratch_shapes=[
            vmem((members, R, C, V), f32),
            vmem((G * pack_rows, O), f32),
            vmem((C * pack_rows, O), f32),
            vmem((R, C, V), f32),
            vmem((R * J * C, O), f32),
            vmem((2 * R, C, O), f32),
            vmem((2 * targets, slots_all), jnp.bfloat16),
            vmem((QP, slots_all), jnp.bfloat16),
            vmem((QP, slots_all), jnp.bfloat16),
            vmem((targets, QP), f32),
            vmem((2, edge_rows, QP), f32),
            vmem((2, 4 * C, QP), f32),
            vmem((6, edge_rows, QP), f32),
            vmem((width, QP), f32),
            vmem((members, J, width), f32),
            vmem((members, J, width), f32),
            vmem((members, J, width), f32),
            vmem((2, J, width), f32),
            vmem((QP, width), f32),
            vmem((members, R, C, V), f32),
            dma((M,)), dma((M,)), dma((G,)), dma((G,)), dma((8,)), dma((8,)), dma((M,)), dma((M,)), dma((3,)),
        ],
        compiler_params=pltpu.CompilerParams(
            collective_id=0, has_side_effects=True, vmem_limit_bytes=56 * 1024 * 1024
        ),
    )(ensemble, flat(obs_value), flat(obs_error), flat(obs_index), obs_count.reshape(1, -1))


def solution(mesh):
    return jax.shard_map(
        functools.partial(local, mesh.shape["member"], mesh.shape["region"]),
        mesh=mesh,
        in_specs=(
            P("member", "region", None, None),
            P(None, ("member", "region"), None),
            P(None, ("member", "region"), None),
            P(None, ("member", "region"), None),
            P(None, ("member", "region")),
        ),
        out_specs=P("member", "region", None, None),
        check_vma=False,
    )
```

```python
import functools
import math

import jax
import jax.numpy as jnp
from jax import lax
from jax.experimental import pallas as pl
from jax.experimental.pallas import tpu as pltpu
from jax.sharding import PartitionSpec as P

SIDE = 16
CELLS = SIDE * SIDE
HALF = SIDE // 2
LANES = 128
NS_ITERS = 6
LOC_SCALE = 12.0
INFLATION_FACTOR = 1.1
MESH = pl.DeviceIdType.MESH
NT = (((1,), (1,)), ((), ()))


def up_to(value, step):
    return -(-value // step) * step


def split(values):
    high = values.astype(jnp.bfloat16)
    low = (values - high.astype(jnp.float32)).astype(jnp.bfloat16)
    return high, low


def kernel(
    dims,
    ens_ref, value_any, error_any, index_any, count_ref, out_ref,
    value_ref, error_ref, index_ref, ens, pack, obs, mean, slots, place, loc, qhi, qlo, acc, side,
    row_in, side_in, prec, root, inv, step, small, weights, outgoing,
    ens_send, ens_recv, obs_send, obs_recv, halo_send, halo_recv, out_send, out_recv, local_sem,
):
    M, G, K, R, C, V, O, J, QP = dims
    members = M * K
    m = lax.axis_index("member")
    g = lax.axis_index("region")
    pack_rows = pack.shape[0] // G
    ts = 2 * (R + 2)
    targets = 4 * C * (R + 2)
    f32 = jnp.float32

    loads = []
    for n, (src, dst) in enumerate(((value_any, value_ref), (error_any, error_ref), (index_any, index_ref))):
        load = pltpu.make_async_copy(src, dst, local_sem.at[3 + n])
        load.start()
        loads.append(load)
    barrier = pltpu.get_barrier_semaphore()
    for off in range(1, M):
        pl.semaphore_signal(barrier, inc=1, device_id=(lax.rem(m + off, M), g), device_id_type=MESH)
    for off in range(1, G):
        pl.semaphore_signal(barrier, inc=1, device_id=(m, lax.rem(g + off, G)), device_id_type=MESH)
    near = {}
    for dm in (-1, 0, 1):
        for dg in (-1, 0, 1):
            if dm == 0 and dg == 0:
                continue
            ok = jnp.bool_(True)
            if dm:
                ok = jnp.logical_and(ok, m > 0 if dm < 0 else m < M - 1)
            if dg:
                ok = jnp.logical_and(ok, g > 0 if dg < 0 else g < G - 1)
            near[dm, dg] = ok
            if dm and dg:
                @pl.when(ok)
                def _():
                    pl.semaphore_signal(barrier, inc=1, device_id=(m + dm, g + dg), device_id_type=MESH)

    own_ens = pltpu.make_async_copy(
        ens_ref.at[:, :, pl.ds(pl.multiple_of(m * C, C), C), :], ens.at[pl.ds(m * K, K)], local_sem.at[0]
    )
    own_ens.start()
    for load in loads:
        load.wait()
    slot = lax.broadcasted_iota(jnp.int32, (G * R, O), 1)
    slot_row = lax.broadcasted_iota(jnp.int32, (G * R, O), 0)
    count = jnp.zeros((G * R, O), jnp.int32)
    for d in range(G * R):
        count = jnp.where(slot_row == d, count_ref[0, d], count)
    live = jnp.where(slot < count, 1.0, 0.0).astype(f32)
    weight = jnp.sqrt(live / error_ref[...])
    value = value_ref[...]
    index_f = index_ref[...].astype(f32)
    for d in range(G):
        base = d * pack_rows
        pack[base : base + R, :] = weight[d * R : (d + 1) * R]
        pack[base + R : base + 2 * R, :] = value[d * R : (d + 1) * R]
        pack[base + 2 * R : base + 3 * R, :] = index_f[d * R : (d + 1) * R]
        if pack_rows > 3 * R:
            pack[base + 3 * R : base + pack_rows, :] = jnp.zeros((pack_rows - 3 * R, O), f32)
    if QP > members * J:
        qhi[members * J :, :] = jnp.zeros((QP - members * J, qhi.shape[1]), jnp.bfloat16)
        qlo[members * J :, :] = jnp.zeros((QP - members * J, qlo.shape[1]), jnp.bfloat16)

    sides = jnp.where(m > 0, 1, 0) + jnp.where(m < M - 1, 1, 0)
    ends = jnp.where(g > 0, 1, 0) + jnp.where(g < G - 1, 1, 0)
    pl.semaphore_wait(barrier, M - 1 + G - 1 + sides * ends)

    sends = []
    for off in range(1, M):
        to = lax.rem(m + off, M)
        copy = pltpu.make_async_remote_copy(
            src_ref=ens_ref.at[:, :, pl.ds(pl.multiple_of(to * C, C), C), :],
            dst_ref=ens.at[pl.ds(m * K, K)],
            send_sem=ens_send.at[off], recv_sem=ens_recv.at[off],
            device_id=(to, g), device_id_type=MESH,
        )
        copy.start()
        sends.append(copy)
    own_row = pl.ds(pl.multiple_of(g * pack_rows, pack_rows), pack_rows)
    own_obs = pltpu.make_async_copy(pack.at[own_row], obs.at[own_row], local_sem.at[1])
    own_obs.start()
    for off in range(1, G):
        to = lax.rem(g + off, G)
        copy = pltpu.make_async_remote_copy(
            src_ref=pack.at[pl.ds(pl.multiple_of(to * pack_rows, pack_rows), pack_rows)],
            dst_ref=obs.at[own_row],
            send_sem=obs_send.at[off], recv_sem=obs_recv.at[off],
            device_id=(m, to), device_id_type=MESH,
        )
        copy.start()
        sends.append(copy)
    own_ens.wait()
    own_obs.wait()
    for off in range(1, M):
        came = lax.rem(m + M - off, M)
        pltpu.make_async_remote_copy(
            src_ref=ens_ref.at[:, :, pl.ds(pl.multiple_of(m * C, C), C), :],
            dst_ref=ens.at[pl.ds(came * K, K)],
            send_sem=ens_send.at[off], recv_sem=ens_recv.at[off],
            device_id=(came, g), device_id_type=MESH,
        ).wait_recv()
    for off in range(1, G):
        came = lax.rem(g + G - off, G)
        pltpu.make_async_remote_copy(
            src_ref=pack.at[own_row],
            dst_ref=obs.at[pl.ds(pl.multiple_of(came * pack_rows, pack_rows), pack_rows)],
            send_sem=obs_send.at[off], recv_sem=obs_recv.at[off],
            device_id=(m, came), device_id_type=MESH,
        ).wait_recv()

    tiles = V // LANES
    for i in range(R):
        wgt = obs[pl.ds(i, C, stride=pack_rows), :]
        val = obs[pl.ds(R + i, C, stride=pack_rows), :]
        idx = obs[pl.ds(2 * R + i, C, stride=pack_rows), :].astype(jnp.int32)
        lane = idx & (LANES - 1)
        tile = idx >> 7
        cell = idx & (CELLS - 1)
        place[2 * i] = (cell >> 4).astype(f32)
        place[2 * i + 1] = (cell & (SIDE - 1)).astype(f32)

        def seen(rows):
            got = jnp.take_along_axis(rows[:, :LANES], lane, axis=1)
            for t in range(1, tiles):
                more = jnp.take_along_axis(rows[:, t * LANES : (t + 1) * LANES], lane, axis=1)
                got = jnp.where(tile == t, more, got)
            return got

        total = ens[0, i]
        for k in range(1, members):
            total = total + ens[k, i]
        avg = total * (1.0 / members)
        mean[i] = avg
        seen_mean = seen(avg)
        base = i * J * C
        for k in range(members):
            slots[base + k * C : base + (k + 1) * C, :] = wgt * (seen(ens[k, i]) - seen_mean)
        slots[base + members * C : base + (members + 1) * C, :] = wgt * (val - seen_mean)
        if J > members + 1:
            slots[base + (members + 1) * C : base + J * C, :] = jnp.zeros(((J - members - 1) * C, O), f32)

    scale = -1.0 / (2.0 * LOC_SCALE * LOC_SCALE)
    middle = (HALF - 1) * 0.5
    t_id = lax.broadcasted_iota(jnp.int32, (ts, O), 0)
    t_row = t_id >> 1
    t_mid = (t_id & 1).astype(f32) * HALF + middle
    col = lax.broadcasted_iota(jnp.int32, (C, O), 0)
    edges = {0: [None] * R, 1: [None] * R}
    for c in range(C):
        for i in range(R):
            at = (c * R + i) * O
            here = slots[pl.ds(i * J * C + c, J, stride=C), :]
            prod = jnp.concatenate([here[k : k + 1] * here for k in range(members)], axis=0)
            high, low = split(prod)
            qhi[0 : members * J, at : at + O] = high
            qlo[0 : members * J, at : at + O] = low
            y = place[2 * i, c : c + 1, :]
            x = place[2 * i + 1, c : c + 1, :]
            row_off = i + 1 - t_row
            dy = (row_off * SIDE).astype(f32) + y - t_mid
            ly = jnp.where(jnp.abs(row_off) <= 1, jnp.exp(dy * dy * scale), 0.0)
            col_off = c - col
            lx = []
            for pc in range(2):
                dx = (col_off * SIDE).astype(f32) + x - (pc * HALF + middle)
                lx.append(jnp.where(jnp.abs(col_off) <= 1, jnp.exp(dx * dx * scale), 0.0))
            grid = jnp.concatenate([ly[s : s + 1] * lx[pc] for s in range(ts) for pc in range(2)], axis=0)
            high, low = split(grid)
            loc[0:targets, at : at + O] = high
            loc[targets : 2 * targets, at : at + O] = low
            for which, away, at_col in ((0, 1, 0), (1, -1, C - 1)):
                if c == at_col:
                    parts = []
                    for pc in range(2):
                        dx = away * SIDE + x - (pc * HALF + middle)
                        parts.append(ly * jnp.exp(dx * dx * scale))
                    edges[which][i] = jnp.concatenate(parts, axis=0)

    def dot(left, right):
        return lax.dot_general(left, right, NT, preferred_element_type=f32)

    for which, first in ((0, 0), (1, (C - 1) * R * O)):
        high, low = split(jnp.concatenate(edges[which], axis=1))
        hq = qhi[:, first : first + R * O]
        side[which] = dot(high, hq) + dot(low, hq) + dot(high, qlo[:, first : first + R * O])
    both = dot(loc[...], qhi[...])
    acc[...] = both[:targets] + both[targets:] + dot(loc[0:targets, :], qlo[...])

    rows = 4 * C
    plans = []
    for n, (dm, dg) in enumerate(near):
        if dm == 0:
            first = 0 if dg < 0 else (R + 1) * rows
            src = acc.at[first : first + rows]
            dst = row_in.at[0 if dg < 0 else 1]
        else:
            src = side.at[0 if dm < 0 else 1]
            dst = side_in.at[(0 if dm < 0 else 3) + dg + 1]
        plans.append((dm, dg, src, dst, n))
    for dm, dg, src, dst, n in plans:
        @pl.when(near[dm, dg])
        def _():
            pltpu.make_async_remote_copy(
                src_ref=src, dst_ref=dst, send_sem=halo_send.at[n], recv_sem=halo_recv.at[n],
                device_id=(m + dm, g + dg), device_id_type=MESH,
            ).start()
    for dm, dg, src, dst, n in plans:
        @pl.when(near[-dm, -dg])
        def _():
            pltpu.make_async_remote_copy(
                src_ref=src, dst_ref=dst, send_sem=halo_send.at[n], recv_sem=halo_recv.at[n],
                device_id=(m - dm, g - dg), device_id_type=MESH,
            ).wait_recv()

        @pl.when(jnp.logical_not(near[-dm, -dg]))
        def _():
            dst[...] = jnp.zeros(dst.shape, f32)

    sub = lax.broadcasted_iota(jnp.int32, (C, QP), 0)
    own = R * rows
    for i in range(R):
        for pr in range(2):
            for pc in range(2):
                first = (i * 4 + pr * 2 + pc) * C
                block = acc[rows + first : rows + first + C, :]
                if i == R - 1:
                    block = block + row_in[0, (pr * 2 + pc) * C : (pr * 2 + pc + 1) * C, :]
                if i == 0:
                    block = block + row_in[1, (pr * 2 + pc) * C : (pr * 2 + pc + 1) * C, :]
                for base, at_col in ((0, C - 1), (3, 0)):
                    def pick(dg, t):
                        place_in = pc * ts + t * 2 + pr
                        return side_in[base + dg + 1, place_in : place_in + 1, :]

                    line = pick(0, i + 1)
                    if i == R - 1:
                        line = line + pick(-1, 0)
                    if i == 0:
                        line = line + pick(1, R + 1)
                    block = block + jnp.where(sub == at_col, line, 0.0)
                prec[first : first + C, :] = block
    width = prec.shape[0]
    if width > own:
        prec[own:, :] = jnp.zeros((width - own, QP), f32)

    flat = jnp.transpose(prec[...])
    j_id = lax.broadcasted_iota(jnp.int32, (J, width), 0)
    eye = [jnp.where(j_id == k, 1.0, 0.0).astype(f32) for k in range(members)]
    drive = []
    mats = []
    squares = None
    for k in range(members):
        line = flat[k * J : (k + 1) * J]
        drive.append(line[members : members + 1])
        mat = jnp.where(j_id < members, line, 0.0) + ((members - 1) / INFLATION_FACTOR) * eye[k]
        mats.append(mat)
        squares = mat * mat if squares is None else squares + mat * mat
    norm = jnp.sqrt(jnp.sum(squares, axis=0, keepdims=True))
    for k in range(members):
        start = mats[k] / norm
        first_m = 1.5 * eye[k] - 0.5 * start
        root[k] = start
        step[k] = first_m
        inv[k] = first_m

    def times(left, k, right):
        out = left[k, 0:1, :] * right[0]
        for i in range(1, members):
            out = out + left[k, i : i + 1, :] * right[i]
        return out

    def apply(*lefts):
        right = [step[i] for i in range(members)]
        for k in range(members):
            for left in lefts:
                left[k] = times(left, k, right)

    def next_step():
        right = [root[i] for i in range(members)]
        for k in range(members):
            step[k] = 1.5 * jnp.where(j_id == k, 1.0, 0.0) - 0.5 * times(inv, k, right)

    apply(root)

    def sweep(_, carry):
        next_step()
        apply(root, inv)
        return carry

    lax.fori_loop(0, NS_ITERS - 2, sweep, 0)
    next_step()
    apply(inv)
    shrink = 1.0 / jnp.sqrt(norm)
    inv_root = [inv[k] * shrink for k in range(members)]
    half_way = drive[0] * inv_root[0]
    for i in range(1, members):
        half_way = half_way + drive[i] * inv_root[i]
    small[0] = half_way
    mean_w = small[0, 0:1, :] * inv_root[0]
    for i in range(1, members):
        mean_w = mean_w + small[0, i : i + 1, :] * inv_root[i]
    small[1] = mean_w
    for j in range(members):
        weights[j * J : (j + 1) * J, :] = small[1, j : j + 1, :] + math.sqrt(members - 1) * inv_root[j]
    if QP > members * J:
        weights[members * J :, :] = jnp.zeros((QP - members * J, width), f32)
    prec[...] = jnp.transpose(weights[...])

    fields = V // CELLS
    band = HALF * SIDE
    left_half = (lax.broadcasted_iota(jnp.int32, (C, band), 1) & (SIDE - 1)) < HALF
    def update(dest):
        for i in range(R):
            for h in range(2):
                first = (i * 4 + 2 * h) * C
                west = prec[first : first + C, :]
                east = prec[first + C : first + 2 * C, :]
                lanes = [f * CELLS + h * band for f in range(fields)]
                avgs = [mean[i, :, a : a + band] for a in lanes]
                outs = [[avgs[f] for f in range(fields)] for _ in range(K)]
                for j in range(members):
                    anoms = [ens[j, i, :, a : a + band] - avgs[f] for f, a in enumerate(lanes)]
                    for kk in range(K):
                        q = j * J + dest * K + kk
                        w = jnp.where(
                            left_half,
                            jnp.broadcast_to(west[:, q : q + 1], (C, band)),
                            jnp.broadcast_to(east[:, q : q + 1], (C, band)),
                        )
                        for f in range(fields):
                            outs[kk][f] = outs[kk][f] + anoms[f] * w
                for kk in range(K):
                    for f, a in enumerate(lanes):
                        outgoing[dest * K + kk, i, :, a : a + band] = outs[kk][f]
        away = lax.rem(dest - m + M, M)
        target = out_ref.at[:, :, pl.ds(pl.multiple_of(m * C, C), C), :]

        @pl.when(away != 0)
        def _():
            pltpu.make_async_remote_copy(
                src_ref=outgoing.at[dest * K : (dest + 1) * K], dst_ref=target,
                send_sem=out_send.at[away], recv_sem=out_recv.at[away],
                device_id=(dest, g), device_id_type=MESH,
            ).start()

        @pl.when(away == 0)
        def _():
            pltpu.make_async_copy(outgoing.at[dest * K : (dest + 1) * K], target, local_sem.at[2]).start()

    far = M // 2

    @pl.when(m < far)
    def _():
        for dest in list(range(far, M)) + list(range(far)):
            update(dest)

    @pl.when(m >= far)
    def _():
        for dest in range(M):
            update(dest)

    for copy in sends:
        copy.wait_send()
    for dm, dg, src, dst, n in plans:
        @pl.when(near[dm, dg])
        def _():
            pltpu.make_async_remote_copy(
                src_ref=src, dst_ref=dst, send_sem=halo_send.at[n], recv_sem=halo_recv.at[n],
                device_id=(m + dm, g + dg), device_id_type=MESH,
            ).wait_send()
    pltpu.make_async_copy(
        outgoing.at[pl.ds(m * K, K)], out_ref.at[:, :, pl.ds(pl.multiple_of(m * C, C), C), :], local_sem.at[2]
    ).wait()
    for off in range(1, M):
        to = lax.rem(m + off, M)
        came = lax.rem(m + M - off, M)
        pltpu.make_async_remote_copy(
            src_ref=outgoing.at[pl.ds(to * K, K)],
            dst_ref=out_ref.at[:, :, pl.ds(pl.multiple_of(came * C, C), C), :],
            send_sem=out_send.at[off], recv_sem=out_recv.at[off],
            device_id=(to, g), device_id_type=MESH,
        ).wait()


def local(M, G, ensemble, obs_value, obs_error, obs_index, obs_count):
    K, R, cols, V = ensemble.shape
    O = obs_value.shape[2]
    C = cols // M
    members = M * K
    J = up_to(members + 1, 8)
    QP = up_to(members * J, LANES)
    slots_all = R * C * O
    targets = 4 * C * (R + 2)
    width = up_to(4 * C * R, LANES)
    pack_rows = up_to(3 * R, 8)
    f32 = jnp.float32
    vmem = pltpu.VMEM
    edge_rows = 4 * (R + 2)
    dma = pltpu.SemaphoreType.DMA
    flat = lambda a: a.reshape(a.shape[0], -1)
    return pl.pallas_call(
        functools.partial(kernel, (M, G, K, R, C, V, O, J, QP)),
        out_shape=pltpu.VMEM(ensemble.shape, f32),
        in_specs=[pl.BlockSpec(memory_space=pl.ANY)] * 4
        + [pl.BlockSpec(memory_space=pltpu.SMEM)],
        out_specs=pl.BlockSpec(memory_space=vmem),
        scratch_shapes=[
            vmem((G * R, O), f32),
            vmem((G * R, O), f32),
            vmem((G * R, O), jnp.int32),
            vmem((members, R, C, V), f32),
            vmem((G * pack_rows, O), f32),
            vmem((C * pack_rows, O), f32),
            vmem((R, C, V), f32),
            vmem((R * J * C, O), f32),
            vmem((2 * R, C, O), f32),
            vmem((2 * targets, slots_all), jnp.bfloat16),
            vmem((QP, slots_all), jnp.bfloat16),
            vmem((QP, slots_all), jnp.bfloat16),
            vmem((targets, QP), f32),
            vmem((2, edge_rows, QP), f32),
            vmem((2, 4 * C, QP), f32),
            vmem((6, edge_rows, QP), f32),
            vmem((width, QP), f32),
            vmem((members, J, width), f32),
            vmem((members, J, width), f32),
            vmem((members, J, width), f32),
            vmem((2, J, width), f32),
            vmem((QP, width), f32),
            vmem((members, R, C, V), f32),
            dma((M,)), dma((M,)), dma((G,)), dma((G,)), dma((8,)), dma((8,)), dma((M,)), dma((M,)), dma((6,)),
        ],
        compiler_params=pltpu.CompilerParams(
            collective_id=0, has_side_effects=True, vmem_limit_bytes=56 * 1024 * 1024
        ),
    )(ensemble, flat(obs_value), flat(obs_error), flat(obs_index), obs_count.reshape(1, -1))


def solution(mesh):
    return jax.shard_map(
        functools.partial(local, mesh.shape["member"], mesh.shape["region"]),
        mesh=mesh,
        in_specs=(
            P("member", "region", None, None),
            P(None, ("member", "region"), None),
            P(None, ("member", "region"), None),
            P(None, ("member", "region"), None),
            P(None, ("member", "region")),
        ),
        out_specs=P("member", "region", None, None),
        check_vma=False,
    )
```

```python
import functools
import math

import jax
import jax.numpy as jnp
from jax import lax
from jax.experimental import pallas as pl
from jax.experimental.pallas import tpu as pltpu
from jax.sharding import PartitionSpec as P

SIDE = 16
CELLS = SIDE * SIDE
HALF = SIDE // 2
LANES = 128
NS_ITERS = 6
LOC_SCALE = 12.0
INFLATION_FACTOR = 1.1
MESH = pl.DeviceIdType.MESH
NT = (((1,), (1,)), ((), ()))


def up_to(value, step):
    return -(-value // step) * step


def split(values):
    high = values.astype(jnp.bfloat16)
    low = (values - high.astype(jnp.float32)).astype(jnp.bfloat16)
    return high, low


def kernel(
    dims,
    ens_ref, value_any, error_any, index_any, count_ref, out_ref,
    value_ref, error_ref, index_ref, ens, pack, obs, slots, place, loc, qhi, qlo, acc, side,
    row_in, side_in, prec, root, inv, step, small, weights, came_weights,
    ens_send, ens_recv, obs_send, obs_recv, halo_send, halo_recv, out_send, out_recv,
    far_send, far_recv, pair_send, pair_recv, local_sem,
):
    M, G, K, R, C, V, O, J, QP = dims
    members = M * K
    m = lax.axis_index("member")
    g = lax.axis_index("region")
    pack_rows = pack.shape[0] // G
    ts = 2 * (R + 2)
    targets = 4 * C * (R + 2)
    f32 = jnp.float32

    loads = []
    for n, (src, dst) in enumerate(((value_any, value_ref), (error_any, error_ref), (index_any, index_ref))):
        load = pltpu.make_async_copy(src, dst, local_sem.at[3 + n])
        load.start()
        loads.append(load)
    barrier = pltpu.get_barrier_semaphore()
    for off in range(1, M):
        pl.semaphore_signal(barrier, inc=1, device_id=(lax.rem(m + off, M), g), device_id_type=MESH)
    for off in range(1, G):
        pl.semaphore_signal(barrier, inc=1, device_id=(m, lax.rem(g + off, G)), device_id_type=MESH)
    near = {}
    for dm in (-1, 0, 1):
        for dg in (-1, 0, 1):
            if dm == 0 and dg == 0:
                continue
            ok = jnp.bool_(True)
            if dm:
                ok = jnp.logical_and(ok, m > 0 if dm < 0 else m < M - 1)
            if dg:
                ok = jnp.logical_and(ok, g > 0 if dg < 0 else g < G - 1)
            near[dm, dg] = ok
            if dm and dg:
                @pl.when(ok)
                def _():
                    pl.semaphore_signal(barrier, inc=1, device_id=(m + dm, g + dg), device_id_type=MESH)

    own_ens = pltpu.make_async_copy(
        ens_ref, ens.at[pl.ds(m * K, K)], local_sem.at[0]
    )
    own_ens.start()
    for load in loads:
        load.wait()
    slot = lax.broadcasted_iota(jnp.int32, (G * R, O), 1)
    slot_row = lax.broadcasted_iota(jnp.int32, (G * R, O), 0)
    count = jnp.zeros((G * R, O), jnp.int32)
    for d in range(G * R):
        count = jnp.where(slot_row == d, count_ref[0, d], count)
    live = jnp.where(slot < count, 1.0, 0.0).astype(f32)
    weight = jnp.sqrt(live / error_ref[...])
    value = value_ref[...]
    index_f = index_ref[...].astype(f32)
    for d in range(G):
        base = d * pack_rows
        pack[base : base + R, :] = weight[d * R : (d + 1) * R]
        pack[base + R : base + 2 * R, :] = value[d * R : (d + 1) * R]
        pack[base + 2 * R : base + 3 * R, :] = index_f[d * R : (d + 1) * R]
        if pack_rows > 3 * R:
            pack[base + 3 * R : base + pack_rows, :] = jnp.zeros((pack_rows - 3 * R, O), f32)
    if weights.shape[1] > members * K:
        tail = weights.shape[1] - members * K
        weights[:, members * K :, :] = jnp.zeros((M, tail, weights.shape[2]), f32)
    if QP > members * J:
        qhi[members * J :, :] = jnp.zeros((QP - members * J, qhi.shape[1]), jnp.bfloat16)
        qlo[members * J :, :] = jnp.zeros((QP - members * J, qlo.shape[1]), jnp.bfloat16)

    sides = jnp.where(m > 0, 1, 0) + jnp.where(m < M - 1, 1, 0)
    ends = jnp.where(g > 0, 1, 0) + jnp.where(g < G - 1, 1, 0)
    pl.semaphore_wait(barrier, M - 1 + G - 1 + sides * ends)

    def block(ref, owner, group):
        columns = pl.ds(pl.multiple_of(group * C, C), C)
        if owner is None:
            return ref.at[:, :, columns, :]
        return ref.at[pl.ds(owner * K, K), :, columns, :]

    def move(src, dst, to, send, recv, n):
        return pltpu.make_async_remote_copy(
            src_ref=src, dst_ref=dst, send_sem=send.at[n], recv_sem=recv.at[n],
            device_id=(to, g), device_id_type=MESH,
        )

    chips = M // 2
    chip = m // 2
    core = lax.rem(m, 2)
    pal = chip * 2 + 1 - core
    rest_out, rest_in, own_out, own_in, near_out, near_in, last_out, last_in = [[] for _ in range(8)]
    slot_no = 0
    for off in range(1, M):
        group = lax.rem(pal + off, M)
        mine = lax.rem(m + off, M)
        own_out.append(move(block(ens_ref, None, group), block(ens, m, group), pal, pair_send, pair_recv, slot_no))
        own_in.append(move(block(ens_ref, None, mine), block(ens, pal, mine), pal, pair_send, pair_recv, slot_no))
        slot_no += 1
    for co in range(1, chips):
        away = lax.rem(chip + co, chips)
        back = lax.rem(chip + chips - co, chips)
        for flip in range(2):
            lane_core = core if flip == 0 else 1 - core
            pal_core = 1 - core if flip == 0 else core
            near_out.append(move(
                block(ens, away * 2 + lane_core, m), block(ens, away * 2 + lane_core, m),
                pal, pair_send, pair_recv, slot_no,
            ))
            near_in.append(move(
                block(ens, away * 2 + pal_core, pal), block(ens, away * 2 + pal_core, pal),
                pal, pair_send, pair_recv, slot_no,
            ))
            slot_no += 1
        for po in range(1, chips):
            for cc in range(2):
                n = ((co - 1) * (chips - 1) + po - 1) * 2 + cc
                group = lax.rem(away + po, chips) * 2 + cc
                mine = lax.rem(chip + po, chips) * 2 + cc
                rest_out.append(move(
                    block(ens_ref, None, group), block(ens, m, group), away * 2 + core, far_send, far_recv, n
                ))
                rest_in.append(move(
                    block(ens_ref, None, mine), block(ens, back * 2 + core, mine), back * 2 + core, far_send, far_recv, n
                ))
                last_out.append(move(
                    block(ens, back * 2 + core, mine), block(ens, back * 2 + core, mine),
                    pal, pair_send, pair_recv, slot_no,
                ))
                last_in.append(move(
                    block(ens, back * 2 + 1 - core, mine), block(ens, back * 2 + 1 - core, mine),
                    pal, pair_send, pair_recv, slot_no,
                ))
                slot_no += 1

    sends = []
    for off in range(1, M):
        to = lax.rem(m + off, M)
        copy = pltpu.make_async_remote_copy(
            src_ref=ens_ref.at[:, :, pl.ds(pl.multiple_of(to * C, C), C), :],
            dst_ref=block(ens, m, to),
            send_sem=ens_send.at[off], recv_sem=ens_recv.at[off],
            device_id=(to, g), device_id_type=MESH,
        )
        copy.start()
        sends.append(copy)
    own_row = pl.ds(pl.multiple_of(g * pack_rows, pack_rows), pack_rows)
    own_obs = pltpu.make_async_copy(pack.at[own_row], obs.at[own_row], local_sem.at[1])
    own_obs.start()
    for off in range(1, G):
        to = lax.rem(g + off, G)
        copy = pltpu.make_async_remote_copy(
            src_ref=pack.at[pl.ds(pl.multiple_of(to * pack_rows, pack_rows), pack_rows)],
            dst_ref=obs.at[own_row],
            send_sem=obs_send.at[off], recv_sem=obs_recv.at[off],
            device_id=(m, to), device_id_type=MESH,
        )
        copy.start()
        sends.append(copy)
    early = len(rest_out) // 2
    for copy in own_out + rest_out[:early]:
        copy.start()
    own_ens.wait()
    own_obs.wait()
    for off in range(1, M):
        came = lax.rem(m + M - off, M)
        pltpu.make_async_remote_copy(
            src_ref=ens_ref.at[:, :, pl.ds(pl.multiple_of(m * C, C), C), :],
            dst_ref=block(ens, came, m),
            send_sem=ens_send.at[off], recv_sem=ens_recv.at[off],
            device_id=(came, g), device_id_type=MESH,
        ).wait_recv()
    for off in range(1, G):
        came = lax.rem(g + G - off, G)
        pltpu.make_async_remote_copy(
            src_ref=pack.at[own_row],
            dst_ref=obs.at[pl.ds(pl.multiple_of(came * pack_rows, pack_rows), pack_rows)],
            send_sem=obs_send.at[off], recv_sem=obs_recv.at[off],
            device_id=(m, came), device_id_type=MESH,
        ).wait_recv()

    for copy in near_out:
        copy.start()

    tiles = V // LANES
    for i in range(R):
        wgt = obs[pl.ds(i, C, stride=pack_rows), :]
        val = obs[pl.ds(R + i, C, stride=pack_rows), :]
        idx = obs[pl.ds(2 * R + i, C, stride=pack_rows), :].astype(jnp.int32)
        lane = idx & (LANES - 1)
        tile = idx >> 7
        cell = idx & (CELLS - 1)
        place[2 * i] = (cell >> 4).astype(f32)
        place[2 * i + 1] = (cell & (SIDE - 1)).astype(f32)

        def seen(rows):
            got = jnp.take_along_axis(rows[:, :LANES], lane, axis=1)
            for t in range(1, tiles):
                more = jnp.take_along_axis(rows[:, t * LANES : (t + 1) * LANES], lane, axis=1)
                got = jnp.where(tile == t, more, got)
            return got

        here_cols = pl.ds(pl.multiple_of(m * C, C), C)
        total = ens[0, i, here_cols, :]
        for k in range(1, members):
            total = total + ens[k, i, here_cols, :]
        avg = total * (1.0 / members)
        seen_mean = seen(avg)
        base = i * J * C
        for k in range(members):
            slots[base + k * C : base + (k + 1) * C, :] = wgt * (seen(ens[k, i, here_cols, :]) - seen_mean)
        slots[base + members * C : base + (members + 1) * C, :] = wgt * (val - seen_mean)
        if J > members + 1:
            slots[base + (members + 1) * C : base + J * C, :] = jnp.zeros(((J - members - 1) * C, O), f32)

    scale = -1.0 / (2.0 * LOC_SCALE * LOC_SCALE)
    middle = (HALF - 1) * 0.5
    t_id = lax.broadcasted_iota(jnp.int32, (ts, O), 0)
    t_row = t_id >> 1
    t_mid = (t_id & 1).astype(f32) * HALF + middle
    col = lax.broadcasted_iota(jnp.int32, (C, O), 0)
    edges = {0: [None] * R, 1: [None] * R}
    for c in range(C):
        for i in range(R):
            at = (c * R + i) * O
            here = slots[pl.ds(i * J * C + c, J, stride=C), :]
            prod = jnp.concatenate([here[k : k + 1] * here for k in range(members)], axis=0)
            high, low = split(prod)
            qhi[0 : members * J, at : at + O] = high
            qlo[0 : members * J, at : at + O] = low
            y = place[2 * i, c : c + 1, :]
            x = place[2 * i + 1, c : c + 1, :]
            row_off = i + 1 - t_row
            dy = (row_off * SIDE).astype(f32) + y - t_mid
            ly = jnp.where(jnp.abs(row_off) <= 1, jnp.exp(dy * dy * scale), 0.0)
            col_off = c - col
            lx = []
            for pc in range(2):
                dx = (col_off * SIDE).astype(f32) + x - (pc * HALF + middle)
                lx.append(jnp.where(jnp.abs(col_off) <= 1, jnp.exp(dx * dx * scale), 0.0))
            grid = jnp.concatenate([ly[s : s + 1] * lx[pc] for s in range(ts) for pc in range(2)], axis=0)
            high, low = split(grid)
            loc[0:targets, at : at + O] = high
            loc[targets : 2 * targets, at : at + O] = low
            for which, away, at_col in ((0, 1, 0), (1, -1, C - 1)):
                if c == at_col:
                    parts = []
                    for pc in range(2):
                        dx = away * SIDE + x - (pc * HALF + middle)
                        parts.append(ly * jnp.exp(dx * dx * scale))
                    edges[which][i] = jnp.concatenate(parts, axis=0)

    def dot(left, right):
        return lax.dot_general(left, right, NT, preferred_element_type=f32)

    for which, first in ((0, 0), (1, (C - 1) * R * O)):
        high, low = split(jnp.concatenate(edges[which], axis=1))
        hq = qhi[:, first : first + R * O]
        side[which] = dot(high, hq) + dot(low, hq) + dot(high, qlo[:, first : first + R * O])
    both = dot(loc[...], qhi[...])
    acc[...] = both[:targets] + both[targets:] + dot(loc[0:targets, :], qlo[...])

    rows = 4 * C
    plans = []
    for n, (dm, dg) in enumerate(near):
        if dm == 0:
            first = 0 if dg < 0 else (R + 1) * rows
            src = acc.at[first : first + rows]
            dst = row_in.at[0 if dg < 0 else 1]
        else:
            src = side.at[0 if dm < 0 else 1]
            dst = side_in.at[(0 if dm < 0 else 3) + dg + 1]
        plans.append((dm, dg, src, dst, n))
    for dm, dg, src, dst, n in plans:
        @pl.when(near[dm, dg])
        def _():
            pltpu.make_async_remote_copy(
                src_ref=src, dst_ref=dst, send_sem=halo_send.at[n], recv_sem=halo_recv.at[n],
                device_id=(m + dm, g + dg), device_id_type=MESH,
            ).start()
    for copy in rest_out[early:]:
        copy.start()
    for dm, dg, src, dst, n in plans:
        @pl.when(near[-dm, -dg])
        def _():
            pltpu.make_async_remote_copy(
                src_ref=src, dst_ref=dst, send_sem=halo_send.at[n], recv_sem=halo_recv.at[n],
                device_id=(m - dm, g - dg), device_id_type=MESH,
            ).wait_recv()

        @pl.when(jnp.logical_not(near[-dm, -dg]))
        def _():
            dst[...] = jnp.zeros(dst.shape, f32)

    sub = lax.broadcasted_iota(jnp.int32, (C, QP), 0)
    own = R * rows
    for i in range(R):
        for pr in range(2):
            for pc in range(2):
                first = (i * 4 + pr * 2 + pc) * C
                block = acc[rows + first : rows + first + C, :]
                if i == R - 1:
                    block = block + row_in[0, (pr * 2 + pc) * C : (pr * 2 + pc + 1) * C, :]
                if i == 0:
                    block = block + row_in[1, (pr * 2 + pc) * C : (pr * 2 + pc + 1) * C, :]
                for base, at_col in ((0, C - 1), (3, 0)):
                    def pick(dg, t):
                        place_in = pc * ts + t * 2 + pr
                        return side_in[base + dg + 1, place_in : place_in + 1, :]

                    line = pick(0, i + 1)
                    if i == R - 1:
                        line = line + pick(-1, 0)
                    if i == 0:
                        line = line + pick(1, R + 1)
                    block = block + jnp.where(sub == at_col, line, 0.0)
                prec[first : first + C, :] = block
    width = prec.shape[0]
    if width > own:
        prec[own:, :] = jnp.zeros((width - own, QP), f32)

    flat = jnp.transpose(prec[...])
    j_id = lax.broadcasted_iota(jnp.int32, (J, width), 0)
    eye = [jnp.where(j_id == k, 1.0, 0.0).astype(f32) for k in range(members)]
    drive = []
    mats = []
    squares = None
    for k in range(members):
        line = flat[k * J : (k + 1) * J]
        drive.append(line[members : members + 1])
        mat = jnp.where(j_id < members, line, 0.0) + ((members - 1) / INFLATION_FACTOR) * eye[k]
        mats.append(mat)
        squares = mat * mat if squares is None else squares + mat * mat
    norm = jnp.sqrt(jnp.sum(squares, axis=0, keepdims=True))
    for k in range(members):
        start = mats[k] / norm
        first_m = 1.5 * eye[k] - 0.5 * start
        root[k] = start
        step[k] = first_m
        inv[k] = first_m

    def times(left, k, right):
        out = left[k, 0:1, :] * right[0]
        for i in range(1, members):
            out = out + left[k, i : i + 1, :] * right[i]
        return out

    def apply(*lefts):
        right = [step[i] for i in range(members)]
        for k in range(members):
            for left in lefts:
                left[k] = times(left, k, right)

    def next_step():
        right = [root[i] for i in range(members)]
        for k in range(members):
            step[k] = 1.5 * jnp.where(j_id == k, 1.0, 0.0) - 0.5 * times(inv, k, right)

    apply(root)

    def sweep(_, carry):
        next_step()
        apply(root, inv)
        return carry

    lax.fori_loop(0, NS_ITERS - 2, sweep, 0)
    next_step()
    apply(inv)
    shrink = 1.0 / jnp.sqrt(norm)
    inv_root = [inv[k] * shrink for k in range(members)]
    half_way = drive[0] * inv_root[0]
    for i in range(1, members):
        half_way = half_way + drive[i] * inv_root[i]
    small[0] = half_way
    mean_w = small[0, 0:1, :] * inv_root[0]
    for i in range(1, members):
        mean_w = mean_w + small[0, i : i + 1, :] * inv_root[i]
    small[1] = mean_w
    for j in range(members):
        all_k = small[1, j : j + 1, :] + math.sqrt(members - 1) * inv_root[j]
        for dest in range(M):
            weights[dest, j * K : (j + 1) * K, :] = all_k[dest * K : (dest + 1) * K]

    weight_moves = []
    for off in range(1, M):
        to = lax.rem(m + off, M)
        copy = move(weights.at[to], came_weights.at[m], to, out_send, out_recv, off)
        copy.start()
        weight_moves.append(copy)
    for copy in rest_in:
        copy.wait_recv()
    for copy in last_out:
        copy.start()

    fields = V // CELLS
    band = HALF * SIDE
    left_half = (lax.broadcasted_iota(jnp.int32, (C, band), 1) & (SIDE - 1)) < HALF

    def update(group, turned):
        columns = pl.ds(pl.multiple_of(group * C, C), C)
        for i in range(R):
            for h in range(2):
                first = (i * 4 + 2 * h) * C
                west = turned[first : first + C]
                east = turned[first + C : first + 2 * C]
                lanes = [f * CELLS + h * band for f in range(fields)]
                raw = [[ens[j, i, columns, a : a + band] for a in lanes] for j in range(members)]
                avgs = []
                for f in range(fields):
                    total = raw[0][f]
                    for j in range(1, members):
                        total = total + raw[j][f]
                    avgs.append(total * (1.0 / members))
                outs = [[avgs[f] for f in range(fields)] for _ in range(K)]
                for j in range(members):
                    anoms = [raw[j][f] - avgs[f] for f in range(fields)]
                    for kk in range(K):
                        q = j * K + kk
                        w = jnp.where(
                            left_half,
                            jnp.broadcast_to(west[:, q : q + 1], (C, band)),
                            jnp.broadcast_to(east[:, q : q + 1], (C, band)),
                        )
                        for f in range(fields):
                            outs[kk][f] = outs[kk][f] + anoms[f] * w
                for kk in range(K):
                    for f, a in enumerate(lanes):
                        out_ref[kk, i, columns, a : a + band] = outs[kk][f]

    update(m, jnp.transpose(weights[m]))
    for copy in own_in + near_in + last_in:
        copy.wait_recv()
    for off in range(1, M):
        came = lax.rem(m + M - off, M)
        move(weights.at[m], came_weights.at[came], came, out_send, out_recv, off).wait_recv()
        update(came, jnp.transpose(came_weights[came]))

    sends += own_out + rest_out + near_out + last_out + weight_moves
    for copy in sends:
        copy.wait_send()
    for dm, dg, src, dst, n in plans:
        @pl.when(near[dm, dg])
        def _():
            pltpu.make_async_remote_copy(
                src_ref=src, dst_ref=dst, send_sem=halo_send.at[n], recv_sem=halo_recv.at[n],
                device_id=(m + dm, g + dg), device_id_type=MESH,
            ).wait_send()


def local(M, G, ensemble, obs_value, obs_error, obs_index, obs_count):
    K, R, cols, V = ensemble.shape
    O = obs_value.shape[2]
    C = cols // M
    members = M * K
    J = up_to(members + 1, 8)
    QP = up_to(members * J, LANES)
    slots_all = R * C * O
    targets = 4 * C * (R + 2)
    width = up_to(4 * C * R, LANES)
    pack_rows = up_to(3 * R, 8)
    f32 = jnp.float32
    vmem = pltpu.VMEM
    edge_rows = 4 * (R + 2)
    WR = up_to(members * K, 8)
    chips = M // 2
    far = 2 * (chips - 1) ** 2
    pair = M - 1 + 2 * (chips - 1) + far
    dma = pltpu.SemaphoreType.DMA
    flat = lambda a: a.reshape(a.shape[0], -1)
    return pl.pallas_call(
        functools.partial(kernel, (M, G, K, R, C, V, O, J, QP)),
        out_shape=pltpu.VMEM(ensemble.shape, f32),
        in_specs=[pl.BlockSpec(memory_space=pl.ANY)] * 4
        + [pl.BlockSpec(memory_space=pltpu.SMEM)],
        out_specs=pl.BlockSpec(memory_space=vmem),
        scratch_shapes=[
            vmem((G * R, O), f32),
            vmem((G * R, O), f32),
            vmem((G * R, O), jnp.int32),
            vmem((members, R, cols, V), f32),
            vmem((G * pack_rows, O), f32),
            vmem((C * pack_rows, O), f32),
            vmem((R * J * C, O), f32),
            vmem((2 * R, C, O), f32),
            vmem((2 * targets, slots_all), jnp.bfloat16),
            vmem((QP, slots_all), jnp.bfloat16),
            vmem((QP, slots_all), jnp.bfloat16),
            vmem((targets, QP), f32),
            vmem((2, edge_rows, QP), f32),
            vmem((2, 4 * C, QP), f32),
            vmem((6, edge_rows, QP), f32),
            vmem((width, QP), f32),
            vmem((members, J, width), f32),
            vmem((members, J, width), f32),
            vmem((members, J, width), f32),
            vmem((2, J, width), f32),
            vmem((M, WR, width), f32),
            vmem((M, WR, width), f32),
            dma((M,)), dma((M,)), dma((G,)), dma((G,)), dma((8,)), dma((8,)), dma((M,)), dma((M,)),
            dma((far,)), dma((far,)), dma((pair,)), dma((pair,)), dma((6,)),
        ],
        compiler_params=pltpu.CompilerParams(
            collective_id=0, has_side_effects=True, vmem_limit_bytes=56 * 1024 * 1024
        ),
    )(ensemble, flat(obs_value), flat(obs_error), flat(obs_index), obs_count.reshape(1, -1))


def solution(mesh):
    return jax.shard_map(
        functools.partial(local, mesh.shape["member"], mesh.shape["region"]),
        mesh=mesh,
        in_specs=(
            P("member", "region", None, None),
            P(None, ("member", "region"), None),
            P(None, ("member", "region"), None),
            P(None, ("member", "region"), None),
            P(None, ("member", "region")),
        ),
        out_specs=P("member", "region", None, None),
        check_vma=False,
    )
```
